32 devices in a mesh: videos: 1 (over z), frames: 32 (over y, x, core).
Axes of the slice: x: 4, y: 4, z: 1, core: 2. Of those that a mesh axis runs over, the one named last changes fastest.
The devices are a block of a 4x4x8 slice.
Arguments:
- latents: float32 [128, 256, 4], P(('videos', 'frames'))
- slot_mod: float32 [128, 6, 6, 384], P(('videos', 'frames'))
- step_dt: float32 [128], P(('videos', 'frames'))
- new_noise: float32 [4, 256, 4], P('videos')
- w_in: bfloat16 [4, 384], replicated
- spat_qkv: bfloat16 [6, 3, 384, 6, 64], replicated
- spat_out: bfloat16 [6, 6, 64, 384], replicated
- temp_qkv: bfloat16 [6, 3, 384, 6, 64], replicated
- temp_out: bfloat16 [6, 6, 64, 384], replicated
- temp_bias: float32 [6, 6, 9], replicated
- w_up: bfloat16 [6, 384, 1536], replicated
- w_down: bfloat16 [6, 1536, 384], replicated
- w_out: bfloat16 [384, 4], replicated
Outputs:
- output 1: float32 [4, 256, 4], P('videos', 'frames')
- output 2: float32 [128, 256, 4], P(('videos', 'frames'))
All inputs are finite; a program needn't handle non-finite values.
Results may differ from the reference program's by a relative error of at most 0.0064095.
Values are sent between devices in bfloat16 or wider.
A program may use at most 768 MiB of HBM per device.

```python
import jax
import jax.numpy as jnp
from jax import lax

D = 384
HEADS = 6
CH = 4
TOKENS = 256
RADIUS = 4
FRAMES = 128
LAYERS = 6
STEPS = 4
HEAD = D // HEADS
WIDTH = 2 * RADIUS + 1
HIDDEN = 4 * D
NORM_EPS = 1e-6


def setup_inputs(seed: int = 0, part: int = 0) -> dict:
    root_key = jax.random.key(seed)
    shared_keys = jax.random.split(root_key, 9)
    part_keys = jax.random.split(jax.random.fold_in(root_key, part), 4)

    def weight(key_w, out_shape, fan_in):
        return (jax.random.normal(key_w, out_shape, jnp.float32) * fan_in ** -0.5).astype(jnp.bfloat16)

    return {
        'latents': jax.random.normal(part_keys[0], (FRAMES, TOKENS, CH), jnp.float32),
        'slot_mod': 0.5 * jax.random.normal(part_keys[1], (FRAMES, LAYERS, 6, D), jnp.float32),
        'step_dt': jax.random.uniform(part_keys[2], (FRAMES,), jnp.float32, 0.3, 0.6) * STEPS ** -0.5,
        'new_noise': jax.random.normal(part_keys[3], (STEPS, TOKENS, CH), jnp.float32),
        'w_in': weight(shared_keys[0], (CH, D), CH),
        'spat_qkv': weight(shared_keys[1], (LAYERS, 3, D, HEADS, HEAD), D),
        'spat_out': weight(shared_keys[2], (LAYERS, HEADS, HEAD, D), D),
        'temp_qkv': weight(shared_keys[3], (LAYERS, 3, D, HEADS, HEAD), D),
        'temp_out': weight(shared_keys[4], (LAYERS, HEADS, HEAD, D), D),
        'temp_bias': jax.random.normal(shared_keys[5], (LAYERS, HEADS, WIDTH), jnp.float32),
        'w_up': weight(shared_keys[6], (LAYERS, D, HIDDEN), D),
        'w_down': weight(shared_keys[7], (LAYERS, HIDDEN, D), HIDDEN),
        'w_out': weight(shared_keys[8], (D, CH), D * (1 + 3 * LAYERS)),
    }


def project(rows, weight_mat):
    return jnp.dot(rows, weight_mat, preferred_element_type=jnp.float32)


def modulate(x, shift, scale):
    centred = x - jnp.mean(x, axis=-1, keepdims=True)
    variance = jnp.mean(jnp.square(centred), axis=-1, keepdims=True)
    normed = centred * lax.rsqrt(variance + NORM_EPS)
    return (normed * (1.0 + scale) + shift).astype(jnp.bfloat16)


def spatial_frame(x_frame, shift, scale, w_qkv, w_proj):
    u = modulate(x_frame, shift, scale)
    queries = project(u, w_qkv[0].reshape(D, D)).astype(jnp.bfloat16).reshape(TOKENS, HEADS, HEAD)
    key_side = project(u, w_qkv[1].reshape(D, D)).astype(jnp.bfloat16).reshape(TOKENS, HEADS, HEAD)
    value_side = project(u, w_qkv[2].reshape(D, D)).astype(jnp.bfloat16).reshape(TOKENS, HEADS, HEAD)
    scores = jnp.einsum('qhe,khe->hqk', queries.astype(jnp.float32), key_side.astype(jnp.float32)) * HEAD ** -0.5
    prob_mat = jax.nn.softmax(scores, axis=-1).astype(jnp.bfloat16).astype(jnp.float32)
    attended = jnp.einsum('hqk,khe->qhe', prob_mat, value_side.astype(jnp.float32)).astype(jnp.bfloat16)
    return x_frame + project(attended.reshape(TOKENS, D), w_proj.reshape(D, D))


def mlp_frame(x_frame, shift, scale, up_l, down_l):
    u = modulate(x_frame, shift, scale)
    hidden = jax.nn.gelu(project(u, up_l), approximate=True).astype(jnp.bfloat16)
    return x_frame + project(hidden, down_l)


def temporal_all(x, shift, scale, w_qkv, w_proj, rel_table):
    u = modulate(x, shift[:, None, :], scale[:, None, :]).reshape(FRAMES * TOKENS, D)

    def heads_of(which):
        return project(u, w_qkv[which].reshape(D, D)).astype(jnp.bfloat16).reshape(FRAMES, TOKENS, HEADS, HEAD)

    queries = heads_of(0)
    pad_rows = jnp.zeros((RADIUS, TOKENS, HEADS, HEAD), jnp.bfloat16)
    key_pad = jnp.concatenate([pad_rows, heads_of(1), pad_rows], axis=0)
    value_pad = jnp.concatenate([pad_rows, heads_of(2), pad_rows], axis=0)

    def one_frame(slot):
        query_f = lax.dynamic_index_in_dim(queries, slot, 0, keepdims=False).astype(jnp.float32)
        key_win = lax.dynamic_slice_in_dim(key_pad, slot, WIDTH, 0).astype(jnp.float32)
        value_win = lax.dynamic_slice_in_dim(value_pad, slot, WIDTH, 0).astype(jnp.float32)
        near = slot - RADIUS + jnp.arange(WIDTH)
        inside = (near >= 0) & (near < FRAMES)
        scores = jnp.einsum('phe,wphe->phw', query_f, key_win) * HEAD ** -0.5 + rel_table[None]
        scores = jnp.where(inside, scores, -1e30)
        prob_mat = jax.nn.softmax(scores, axis=-1).astype(jnp.bfloat16).astype(jnp.float32)
        return jnp.einsum('phw,wphe->phe', prob_mat, value_win).astype(jnp.bfloat16).reshape(TOKENS, D)

    attended = lax.map(one_frame, jnp.arange(FRAMES))
    return x + project(attended.reshape(FRAMES * TOKENS, D), w_proj.reshape(D, D)).reshape(FRAMES, TOKENS, D)


def reference(latents, slot_mod, step_dt, new_noise, w_in, spat_qkv, spat_out, temp_qkv, temp_out, temp_bias, w_up, w_down, w_out):
    mod_layers = jnp.swapaxes(slot_mod, 0, 1)

    def one_layer(x, layer_args):
        spat_l, sout_l, temp_l, tout_l, bias_l, up_l, down_l, mod_l = layer_args
        x = lax.map(lambda item: spatial_frame(item[0], item[1][0], item[1][1], spat_l, sout_l), (x, mod_l))
        x = temporal_all(x, mod_l[:, 2], mod_l[:, 3], temp_l, tout_l, bias_l)
        x = lax.map(lambda item: mlp_frame(item[0], item[1][4], item[1][5], up_l, down_l), (x, mod_l))
        return x, None

    def one_step(current, noise_frame):
        flat_rows = current.astype(jnp.bfloat16).reshape(FRAMES * TOKENS, CH)
        x = project(flat_rows, w_in).astype(jnp.bfloat16).astype(jnp.float32).reshape(FRAMES, TOKENS, D)
        x = lax.scan(one_layer, x, (spat_qkv, spat_out, temp_qkv, temp_out, temp_bias, w_up, w_down, mod_layers))[0]
        velocity = project(x.astype(jnp.bfloat16).reshape(FRAMES * TOKENS, D), w_out).reshape(FRAMES, TOKENS, CH)
        updated = current + step_dt[:, None, None] * velocity
        return jnp.concatenate([updated[1:], noise_frame[None]], axis=0), updated[0]

    final_z, emitted = lax.scan(one_step, latents, new_noise)
    return emitted, final_z
```

```python
import functools
import math

import jax
import jax.numpy as jnp
from jax import lax
from jax.experimental import pallas as pl
from jax.experimental.pallas import tpu as pltpu
from jax.sharding import PartitionSpec as P

F32 = jnp.float32
BF16 = jnp.bfloat16
NORM_EPS = 1e-6
LOG2E = math.log2(math.e)
MESH = pl.DeviceIdType.MESH
NEG = -1e30


def tdot(lhs, rhs):
    return lax.dot_general(lhs, rhs, (((0,), (0,)), ((), ())), preferred_element_type=F32)


def dot(lhs, rhs):
    return jnp.dot(lhs, rhs, preferred_element_type=F32)


def fold(op, x, rows=8):
    while x.shape[0] > rows and x.shape[0] % 2 == 0 and (x.shape[0] // 2) % 8 == 0:
        half = x.shape[0] // 2
        x = op(x[:half], x[half:])
    return x


def kernel(cfg, z_in, noise, mods, biasb, w_in, w_out, dt, sq_h, so_h, tq_h, to_h, up_h, dn_h,
           e_out, z_out,
           sq, so, tq, to, up, dn, wsem,
           x_ref, u_own, u_halo, send_sem, recv_sem,
           q_own, kv, qkv, o_ref, s_ref, p_ref, hid, part, pp,
           z_ref, z_snd, z_rcv, zsem, e_buf, e_send, e_recv):
    groups, layers, steps, per_dev, heads, radius = cfg
    d = x_ref.shape[1]
    tok = x_ref.shape[2]
    hd = d // heads
    wide = hid.shape[0]
    window = 2 * radius + 1
    lanes = 128
    chunks = tok // lanes
    scale = hd ** -0.5
    me = lax.axis_index('frames')
    left = lax.max(me - 1, 0)
    right = lax.min(me + 1, groups - 1)
    has_left = me > 0
    has_right = me < groups - 1

    pairs = ((sq_h, sq), (so_h, so), (tq_h, tq), (to_h, to), (up_h, up), (dn_h, dn))

    def wcopy(w, l):
        return pltpu.make_async_copy(pairs[w][0].at[l], pairs[w][1].at[l], wsem.at[w, l])

    def startw(l, _):
        for w in range(6):
            wcopy(w, l).start()
        return 0

    lax.fori_loop(0, layers, startw, 0)

    def u_copy(way, par, f):
        return pltpu.make_async_remote_copy(
            src_ref=u_own.at[f], dst_ref=u_halo.at[par, way, f],
            send_sem=send_sem.at[way, f], recv_sem=recv_sem.at[par, way, f],
            device_id={'frames': right if way == 0 else left}, device_id_type=MESH)

    def z_copy():
        return pltpu.make_async_remote_copy(
            src_ref=z_snd, dst_ref=z_rcv, send_sem=zsem.at[0], recv_sem=zsem.at[1],
            device_id={'frames': left}, device_id_type=MESH)

    def e_copy(s, t):
        return pltpu.make_async_remote_copy(
            src_ref=e_buf.at[s], dst_ref=e_buf.at[s], send_sem=e_send.at[s, t], recv_sem=e_recv.at[s],
            device_id={'frames': t}, device_id_type=MESH)

    z_ref[...] = jnp.zeros_like(z_ref)
    for f in range(per_dev):
        z_ref[f, 0:4, :] = z_in[f]
    part[...] = jnp.zeros_like(part)

    @pl.when(jnp.logical_not(has_left))
    def _():
        u_halo[:, 0] = jnp.zeros((2,) + u_halo.shape[2:], BF16)

    @pl.when(jnp.logical_not(has_right))
    def _():
        u_halo[:, 1] = jnp.zeros((2,) + u_halo.shape[2:], BF16)

    def modulated(f, l, first):
        x = x_ref[f]
        mean = jnp.sum(fold(jnp.add, x), axis=0, keepdims=True) * (1.0 / d)
        centred = x - mean
        var = jnp.sum(fold(jnp.add, centred * centred), axis=0, keepdims=True) * (1.0 / d)
        shift = mods[l, f, :, first:first + 1]
        gain = 1.0 + mods[l, f, :, first + 1:first + 2]
        return (centred * lax.rsqrt(var + NORM_EPS) * gain + shift).astype(BF16)

    def spatial(f, l):
        u = modulated(f, l, 0)
        qkv[...] = dot(sq[l], u).astype(BF16)
        for h in range(heads):
            q = qkv[h * hd:(h + 1) * hd, :]
            k = qkv[d + h * hd:d + (h + 1) * hd, :]
            s_ref[h] = tdot(k, q)
        for h in range(heads):
            s = s_ref[h]
            top = jnp.max(fold(jnp.maximum, s), axis=0, keepdims=True)
            e = jnp.exp2((s - top) * (scale * LOG2E))
            total = jnp.sum(fold(jnp.add, e), axis=0, keepdims=True)
            p_ref[h] = (e * (1.0 / total)).astype(BF16)
        for h in range(heads):
            v = qkv[2 * d + h * hd:2 * d + (h + 1) * hd, :]
            o_ref[h * hd:(h + 1) * hd, :] = dot(v, p_ref[h]).astype(BF16)
        x_ref[f] = x_ref[f] + tdot(so[l], o_ref[...])

    def project_temporal(f, l, par):
        u_own[f] = modulated(f, l, 2)
        r = dot(tq[l], u_own[f]).astype(BF16)
        q_own[f] = r[:d]
        kv[par, radius + f] = r[d:]

    def temporal(a, l, par):
        first = me * per_dev + a - radius
        for c in range(chunks):
            ln = slice(c * lanes, (c + 1) * lanes)
            for h in range(heads):
                qf = q_own[a, h * hd:(h + 1) * hd, ln].astype(F32)
                for j in range(window):
                    kf = kv[par, a + j, h * hd:(h + 1) * hd, ln].astype(F32)
                    part[j, c, h * 8:(h + 1) * 8, :] = fold(jnp.add, qf * kf)
            ss = []
            for j in range(window):
                s = part[j, c, pl.ds(0, 8, stride=8), :]
                for r in range(1, 8):
                    s = s + part[j, c, pl.ds(r, 8, stride=8), :]
                ok = (first + j >= 0) & (first + j < groups * per_dev)
                ss.append(jnp.where(ok, s * scale + biasb[l, j], NEG))
            top = functools.reduce(jnp.maximum, ss)
            es = [jnp.exp(s - top) for s in ss]
            inv = 1.0 / functools.reduce(jnp.add, es)
            for j in range(window):
                pp[j, c] = (es[j] * inv).astype(BF16).astype(F32)
        for c in range(chunks):
            ln = slice(c * lanes, (c + 1) * lanes)
            for h in range(heads):
                acc = None
                for j in range(window):
                    vf = kv[par, a + j, d + h * hd:d + (h + 1) * hd, ln].astype(F32)
                    pb = pp[j, c, pl.ds(h, 8, stride=0), :]
                    t = jnp.concatenate([pb] * (hd // 8), axis=0) * vf
                    acc = t if acc is None else acc + t
                o_ref[h * hd:(h + 1) * hd, ln] = acc.astype(BF16)
        x_ref[a] = x_ref[a] + tdot(to[l], o_ref[...])

    def mlp(a, l):
        u = modulated(a, l, 4)
        piece = d
        for c in range(wide // piece):
            h = tdot(up[l, :, c * piece:(c + 1) * piece], u)
            hid[c * piece:(c + 1) * piece, :] = jax.nn.gelu(h, approximate=True).astype(BF16)
        x_ref[a] = x_ref[a] + tdot(dn[l], hid[...])

    def body(it, _):
        lt = lax.rem(it + layers - 1, layers)
        ls = lax.rem(it, layers)
        step = lax.div(it - 1, layers)
        par = lax.rem(it, 2)
        run_t = it > 0
        run_s = it < steps * layers
        wrap = (ls == 0) & run_t

        @pl.when(it < layers)
        def _():
            for w in range(2):
                wcopy(w, ls).wait()
            wcopy(2, ls).wait()

        @pl.when(run_t & (it <= layers))
        def _():
            for w in range(3, 6):
                wcopy(w, lt).wait()

        @pl.when(run_t)
        def _():
            def halo(f, _):
                @pl.when(has_left)
                def _():
                    u_copy(0, 1 - par, f).wait_recv()

                @pl.when(has_right)
                def _():
                    u_copy(1, 1 - par, f).wait_recv()

                u2 = jnp.concatenate([u_halo[1 - par, 0, f], u_halo[1 - par, 1, f]], axis=1)
                r = dot(tq[lt, d:], u2).astype(BF16)
                kv[1 - par, f] = r[:, :tok]
                kv[1 - par, radius + per_dev + f] = r[:, tok:]
                return 0

            lax.fori_loop(0, per_dev, halo, 0)

        def frame(a, _):
            @pl.when(run_t & (a < per_dev))
            def _():
                temporal(a, lt, 1 - par)
                mlp(a, lt)

                @pl.when(has_right)
                def _():
                    u_copy(0, 1 - par, a).wait_send()

                @pl.when(has_left)
                def _():
                    u_copy(1, 1 - par, a).wait_send()

                @pl.when(ls == 0)
                def _():
                    v = dot(w_out[...], x_ref[a].astype(BF16))
                    new = z_ref[a] + dt[a] * v

                    @pl.when(a > 0)
                    def _():
                        z_ref[a - 1] = new

                    @pl.when((a == 0) & has_left)
                    def _():
                        z_snd[...] = new

                    @pl.when((a == 0) & jnp.logical_not(has_left))
                    def _():
                        e_buf[step] = new

            @pl.when(wrap & (a == 1) & has_left)
            def _():
                z_copy().start()

            @pl.when(wrap & (a == 1) & jnp.logical_not(has_left))
            def _():
                def snd(t, _):
                    e_copy(step, t).start()
                    return 0
                lax.fori_loop(1, groups, snd, 0)

            @pl.when(wrap & (a == per_dev))
            def _():
                @pl.when(has_right)
                def _():
                    z_copy().wait_recv()
                    z_ref[per_dev - 1] = z_rcv[...]

                @pl.when(jnp.logical_not(has_right))
                def _():
                    z_ref[per_dev - 1, 0:4, :] = noise[step]

                @pl.when(has_left)
                def _():
                    z_copy().wait_send()

            slot = lax.select(wrap, a - 1, a)

            @pl.when(run_s & (slot >= 0) & (slot < per_dev))
            def _():
                @pl.when(ls == 0)
                def _():
                    x_ref[slot] = tdot(w_in[...], z_ref[slot].astype(BF16)).astype(BF16).astype(F32)

                spatial(slot, ls)
                project_temporal(slot, ls, par)

                @pl.when(has_right)
                def _():
                    u_copy(0, par, slot).start()

                @pl.when(has_left)
                def _():
                    u_copy(1, par, slot).start()

            return 0

        lax.fori_loop(0, per_dev + 1, frame, 0)
        return 0

    lax.fori_loop(0, steps * layers + 1, body, 0)

    for f in range(per_dev):
        z_out[f] = z_ref[f, 0:4, :]

    @pl.when(has_left)
    def _():
        for s in range(steps):
            e_copy(s, 0).wait_recv()

    @pl.when(jnp.logical_not(has_left))
    def _():
        def fin(t, _):
            for s in range(steps):
                e_copy(s, t).wait_send()
            return 0
        lax.fori_loop(1, groups, fin, 0)

    e_out[...] = e_buf[...]


def solution(mesh):
    groups = mesh.shape['frames']
    slot_spec = P(('videos', 'frames'))

    def per_device(latents, slot_mod, step_dt, new_noise, w_in, spat_qkv, spat_out, temp_qkv, temp_out, temp_bias, w_up, w_down, w_out):
        per_dev, tok, ch = latents.shape
        layers, _, d, heads, hd = spat_qkv.shape
        steps = new_noise.shape[0]
        wide = w_up.shape[-1]
        window = temp_bias.shape[-1]
        radius = (window - 1) // 2

        z_t = jnp.swapaxes(latents, 1, 2)
        n_t = jnp.swapaxes(new_noise, 1, 2)
        mods = jnp.transpose(slot_mod, (1, 0, 3, 2))
        bias = jnp.pad(jnp.transpose(temp_bias, (0, 2, 1)), ((0, 0), (0, 0), (0, 8 - heads)))
        biasb = jnp.broadcast_to(bias[..., None], (layers, window, 8, 128))
        w_in8 = jnp.pad(w_in, ((0, 8 - ch), (0, 0)))
        w_out8 = jnp.pad(w_out.T, ((0, 8 - ch), (0, 0)))
        sq = jnp.transpose(spat_qkv, (0, 1, 3, 4, 2)).reshape(layers, 3 * d, d)
        tq = jnp.transpose(temp_qkv, (0, 1, 3, 4, 2)).reshape(layers, 3 * d, d)
        so = spat_out.reshape(layers, d, d)
        to = temp_out.reshape(layers, d, d)

        vm = pl.BlockSpec(memory_space=pltpu.VMEM)
        sm = pl.BlockSpec(memory_space=pltpu.SMEM)
        anys = pl.BlockSpec(memory_space=pl.ANY)
        V = pltpu.VMEM
        DMA = pltpu.SemaphoreType.DMA
        cfg = (groups, layers, steps, per_dev, heads, radius)
        e_all, z_fin = pl.pallas_call(
            functools.partial(kernel, cfg),
            out_shape=(jax.ShapeDtypeStruct((steps, 8, tok), F32), jax.ShapeDtypeStruct((per_dev, ch, tok), F32)),
            in_specs=[vm, vm, vm, vm, vm, vm, sm] + [anys] * 6,
            out_specs=(vm, vm),
            scratch_shapes=[
                V((layers, 3 * d, d), BF16), V((layers, d, d), BF16), V((layers, 3 * d, d), BF16), V((layers, d, d), BF16),
                V((layers, d, wide), BF16), V((layers, wide, d), BF16), DMA((6, layers)),
                V((per_dev, d, tok), F32), V((per_dev, d, tok), BF16), V((2, 2, per_dev, d, tok), BF16),
                DMA((2, per_dev)), DMA((2, 2, per_dev)),
                V((per_dev, d, tok), BF16), V((2, 2 * radius + per_dev, 2 * d, tok), BF16),
                V((3 * d, tok), BF16), V((d, tok), BF16),
                V((heads, tok, tok), F32), V((heads, tok, tok), BF16), V((wide, tok), BF16),
                V((window, tok // 128, 64, 128), F32), V((window, tok // 128, 8, 128), F32),
                V((per_dev, 8, tok), F32), V((8, tok), F32), V((8, tok), F32), DMA((2,)),
                V((steps, 8, tok), F32), DMA((steps, groups)), DMA((steps,)),
            ],
            compiler_params=pltpu.CompilerParams(has_side_effects=True, vmem_limit_bytes=64000000),
            name='fifo',
        )(z_t, n_t, mods, biasb, w_in8, w_out8, step_dt, sq, so, tq, to, w_up, w_down)

        me = lax.axis_index('frames')
        mine = tok // groups
        e_mine = lax.dynamic_slice_in_dim(e_all[:, :ch], me * mine, mine, 2)
        return jnp.swapaxes(e_mine, 1, 2), jnp.swapaxes(z_fin, 1, 2)

    return jax.shard_map(per_device, mesh=mesh, in_specs=(slot_spec, slot_spec, slot_spec, P('videos'), P(), P(), P(), P(), P(), P(), P(), P(), P()), out_specs=(P('videos', 'frames'), slot_spec), check_vma=False)
```

```python
import functools
import math

import jax
import jax.numpy as jnp
from jax import lax
from jax.experimental import pallas as pl
from jax.experimental.pallas import tpu as pltpu
from jax.sharding import PartitionSpec as P

F32 = jnp.float32
BF16 = jnp.bfloat16
NORM_EPS = 1e-6
LOG2E = math.log2(math.e)
MESH = pl.DeviceIdType.MESH
NEG = -1e30


def tdot(lhs, rhs):
    return lax.dot_general(lhs, rhs, (((0,), (0,)), ((), ())), preferred_element_type=F32)


def dot(lhs, rhs):
    return jnp.dot(lhs, rhs, preferred_element_type=F32)


def fold(op, x, rows=8):
    while x.shape[0] > rows and x.shape[0] % 2 == 0 and (x.shape[0] // 2) % 8 == 0:
        half = x.shape[0] // 2
        x = op(x[:half], x[half:])
    return x


def gelu(x):
    half = 0.5 * x
    c = math.sqrt(2.0 / math.pi)
    return half + half * jnp.tanh(x * (c + (c * 0.044715) * (x * x)))


def kernel(cfg, z_in, noise, mods_in, w_in4, w_out4, dt, bias, sq_h, so_h, tq_h, to_h, up_h, dn_h,
           e_out, z_out,
           sq, so, tq, to, up, dn, wsem,
           x_ref, u_own, u_halo, send_sem, recv_sem,
           q_own, kv, qkv, o_s, o_t, x_s, x_t, s_ref, p_ref, hid, part, pp,
           z_ref, z_snd, z_rcv, zsem, e_buf, e_send, e_recv, mods, biasb, w_in, w_out):
    groups, layers, steps, per_dev, heads, radius = cfg
    d = x_ref.shape[1]
    tok = x_ref.shape[2]
    hd = d // heads
    wide = hid.shape[0]
    window = 2 * radius + 1
    lanes = 128
    chunks = tok // lanes
    scale = hd ** -0.5
    me = lax.axis_index('frames')
    left = lax.max(me - 1, 0)
    right = lax.min(me + 1, groups - 1)
    has_left = me > 0

    has_right = me < groups - 1

    pairs = ((sq_h, sq), (so_h, so), (tq_h, tq), (to_h, to), (up_h, up), (dn_h, dn))

    def wcopy(w, l):
        return pltpu.make_async_copy(pairs[w][0].at[l], pairs[w][1].at[l], wsem.at[w, l])

    def startw(l, _):
        for w in range(6):
            wcopy(w, l).start()
        return 0

    startw(0, 0)

    def u_copy(way, par, f):
        return pltpu.make_async_remote_copy(
            src_ref=u_own.at[f], dst_ref=u_halo.at[par, way, f],
            send_sem=send_sem.at[way, f], recv_sem=recv_sem.at[par, way, f],
            device_id={'frames': right if way == 0 else left}, device_id_type=MESH)

    def z_copy():
        return pltpu.make_async_remote_copy(
            src_ref=z_snd, dst_ref=z_rcv, send_sem=zsem.at[0], recv_sem=zsem.at[1],
            device_id={'frames': left}, device_id_type=MESH)

    def e_copy(s, t):
        return pltpu.make_async_remote_copy(
            src_ref=e_buf.at[s], dst_ref=e_buf.at[s], send_sem=e_send.at[s, t], recv_sem=e_recv.at[s],
            device_id={'frames': t}, device_id_type=MESH)

    ch = z_in.shape[1]
    w_in[...] = jnp.concatenate([w_in4[...].astype(F32), jnp.zeros((8 - ch, d), F32)], axis=0).astype(BF16)
    w_out[...] = jnp.concatenate([w_out4[...].astype(F32), jnp.zeros((8 - ch, d), F32)], axis=0).astype(BF16)

    def prepare(l):
        for f in range(per_dev):
            rows = jnp.concatenate([mods_in[l, p, f:f + 1, :] for p in range(6)] + [jnp.zeros((2, d), F32)], axis=0)
            mods[l, f, :, 0:8] = jnp.transpose(rows)
        row = lax.broadcasted_iota(jnp.int32, (8, lanes), 0)
        for j in range(window):
            tile = jnp.zeros((8, lanes), F32)
            for h in range(heads):
                tile = jnp.where(row == h, bias[l * heads * window + h * window + j], tile)
            biasb[l, j] = tile

    z_ref[...] = jnp.zeros_like(z_ref)
    for f in range(per_dev):
        z_ref[f, 0:4, :] = z_in[f]
    part[...] = jnp.zeros_like(part)

    @pl.when(jnp.logical_not(has_left))
    def _():
        u_halo[:, 0] = jnp.zeros((2,) + u_halo.shape[2:], BF16)

    @pl.when(jnp.logical_not(has_right))
    def _():
        u_halo[:, 1] = jnp.zeros((2,) + u_halo.shape[2:], BF16)

    def modulated(x, f, l, first):
        mean = jnp.sum(fold(jnp.add, x), axis=0, keepdims=True) * (1.0 / d)
        centred = x - mean
        var = jnp.sum(fold(jnp.add, centred * centred), axis=0, keepdims=True) * (1.0 / d)
        shift = mods[l, f, :, first:first + 1]
        gain = 1.0 + mods[l, f, :, first + 1:first + 2]
        return (centred * lax.rsqrt(var + NORM_EPS) * gain + shift).astype(BF16)

    def spatial(f, l):
        u = modulated(x_ref[f], f, l, 0)
        yield 200
        for i in range(6):
            rows = slice(i * (d // 2), (i + 1) * (d // 2))
            qkv[rows, :] = dot(sq[l, rows, :], u).astype(BF16)
            yield 100
        for h in range(heads):
            q = qkv[h * hd:(h + 1) * hd, :]
            k = qkv[d + h * hd:d + (h + 1) * hd, :]
            s_ref[h] = tdot(k, q)
            yield 80
        for h in range(heads):
            s = s_ref[h]
            top = jnp.max(fold(jnp.maximum, s), axis=0, keepdims=True)
            e = jnp.exp2((s - top) * (scale * LOG2E))
            total = jnp.sum(fold(jnp.add, e), axis=0, keepdims=True)
            p_ref[h] = (e * (1.0 / total)).astype(BF16)
            yield 150
        for h in range(heads):
            v = qkv[2 * d + h * hd:2 * d + (h + 1) * hd, :]
            o_s[h * hd:(h + 1) * hd, :] = dot(v, p_ref[h]).astype(BF16)
            yield 80
        x_s[...] = x_ref[f] + tdot(so[l], o_s[...])
        yield 200
        u_own[f] = modulated(x_s[...], f, l, 2)
        x_ref[f] = x_s[...]
        yield 200

    def scores(keys):
        for c in range(chunks):
            ln = slice(c * lanes, (c + 1) * lanes)
            for h in range(heads):
                hs = slice(h * hd, (h + 1) * hd)
                qf = [q_own[a, hs, ln].astype(F32) for a in range(per_dev)]
                for key in keys:
                    kf = kv[key, hs, ln].astype(F32)
                    for a in range(per_dev):
                        if 0 <= key - a < window:
                            part[a, key - a, c, h * 8:(h + 1) * 8, :] = fold(jnp.add, qf[a] * kf)
                yield 1

    def own(l):
        for f in range(0, per_dev, 2):
            u2 = jnp.concatenate([u_own[f], u_own[f + 1]], axis=1)
            for i in range(3):
                r = dot(tq[l, i * d:(i + 1) * d], u2).astype(BF16)
                for g in range(2):
                    if i == 0:
                        q_own[f + g] = r[:, g * tok:(g + 1) * tok]
                    else:
                        kv[radius + f + g, (i - 1) * d:i * d] = r[:, g * tok:(g + 1) * tok]
                yield 1

    def halo(l, par, frames, ways=(0, 1)):
        for f in frames:
            u2 = jnp.concatenate([u_halo[par, way, f] for way in ways], axis=1)
            for i in range(2):
                r = dot(tq[l, (i + 1) * d:(i + 2) * d], u2).astype(BF16)
                for n, way in enumerate(ways):
                    kv[way * (radius + per_dev) + f, i * d:(i + 1) * d] = r[:, n * tok:(n + 1) * tok]
                yield 1

    def temporal_mlp(a, l):
        first = me * per_dev + a - radius
        for c in range(chunks):
            ss = []
            for j in range(window):
                s = part[a, j, c, pl.ds(0, 8, stride=8), :]
                for r in range(1, 8):
                    s = s + part[a, j, c, pl.ds(r, 8, stride=8), :]
                ok = (first + j >= 0) & (first + j < groups * per_dev)
                ss.append(jnp.where(ok, s * scale + biasb[l, j], NEG))
            top = functools.reduce(jnp.maximum, ss)
            es = [jnp.exp(s - top) for s in ss]
            inv = 1.0 / functools.reduce(jnp.add, es)
            for j in range(window):
                pp[j, c] = (es[j] * inv).astype(BF16).astype(F32)
            yield 60
        for c in range(chunks):
            ln = slice(c * lanes, (c + 1) * lanes)
            for h in range(heads):
                acc = None
                for j in range(window):
                    vf = kv[a + j, d + h * hd:d + (h + 1) * hd, ln].astype(F32)
                    pb = pp[j, c, pl.ds(h, 8, stride=0), :]
                    t = jnp.concatenate([pb] * (hd // 8), axis=0) * vf
                    acc = t if acc is None else acc + t
                o_t[h * hd:(h + 1) * hd, ln] = acc.astype(BF16)
                yield 60
        x_t[...] = x_ref[a] + tdot(to[l], o_t[...])
        yield 200
        u = modulated(x_t[...], a, l, 4)
        yield 200
        piece = d
        n = wide // piece
        hs = []
        for c in range(n + 1):
            if c < n:
                hs.append(tdot(up[l, :, c * piece:(c + 1) * piece], u))
                yield 200
            if c > 0:
                hid[(c - 1) * piece:c * piece, :] = gelu(hs[c - 1]).astype(BF16)
                yield 200
        x_ref[a] = x_t[...] + tdot(dn[l], hid[...])
        yield 600

    def run(frame, *streams):
        live = [[g, total, 0.0] for g, total in streams]
        block = frame
        while live:
            block = block + 1

            @pl.when(lax.rem(block * (block + 1), 2) == 0)
            def _():
                waiting = list(live)
                while waiting:
                    entry = min(waiting, key=lambda t: t[2])
                    try:
                        cost = next(entry[0])
                    except StopIteration:
                        waiting.remove(entry)
                        live.remove(entry)
                        continue
                    if cost is None:
                        waiting.remove(entry)
                    else:
                        entry[2] += cost / entry[1]

    S_COST = 1.3 * (200 + 600 + 480 + 900 + 480 + 400)
    T_COST = 60 * 14 + 400 + 1600 + 600

    def body(it, _):
        lt = lax.rem(it + layers - 1, layers)
        ls = lax.rem(it, layers)
        step = lax.div(it - 1, layers)
        par = lax.rem(it, 2)
        run_t = it > 0
        run_s = it < steps * layers
        wrap = (ls == 0) & run_t

        @pl.when(it < layers - 1)
        def _():
            startw(it + 1, 0)

        @pl.when(it < layers)
        def _():
            prepare(ls)
            for w in range(2):
                wcopy(w, ls).wait()

        @pl.when(run_t & (it <= layers))
        def _():
            for w in range(2, 6):
                wcopy(w, lt).wait()

        def arrived(f, ways=(0, 1)):
            for way in ways:
                @pl.when((has_left, has_right)[way])
                def _():
                    u_copy(way, 1 - par, f).wait_recv()

        @pl.when(run_t)
        def _():
            mine = [radius + f for f in range(per_dev)]
            far = radius + per_dev
            run(it, (own(lt), 6))
            arrived(0)
            arrived(1)
            run(it, (halo(lt, 1 - par, (0, 1)), 4), (scores(mine), 12))
            run(it + 1, (scores((0, 1, far, far + 1)), 12))
            arrived(2)
            run(it, (halo(lt, 1 - par, (2,)), 2))
            run(it + 1, (scores((2, far + 2)), 12))
            arrived(3, (0,))
            run(it, (halo(lt, 1 - par, (3,), (0,)), 2))
            run(it + 1, (scores((3,)), 12))

        def pre_t(a):
            @pl.when(a == per_dev - 1)
            def _():
                arrived(per_dev - 1, (1,))
                run(it, (halo(lt, 1 - par, (per_dev - 1,), (1,)), 2))
                run(it + 1, (scores((radius + 2 * per_dev - 1,)), 12))

            @pl.when(has_right)
            def _():
                u_copy(0, 1 - par, a).wait_send()

            @pl.when(has_left)
            def _():
                u_copy(1, 1 - par, a).wait_send()

        def post_t(a):
            @pl.when(ls == 0)
            def _():
                v = dot(w_out[...], x_ref[a].astype(BF16))
                new = z_ref[a] + dt[a] * v

                @pl.when(a > 0)
                def _():
                    z_ref[a - 1] = new

                @pl.when((a == 0) & has_left)
                def _():
                    z_snd[...] = new

                @pl.when((a == 0) & jnp.logical_not(has_left))
                def _():
                    e_buf[step] = new

                @pl.when((a == 1) & has_left)
                def _():
                    z_copy().start()

                @pl.when((a == 1) & jnp.logical_not(has_left))
                def _():
                    def snd(t, _):
                        e_copy(step, t).start()
                        return 0
                    lax.fori_loop(1, groups, snd, 0)

                @pl.when(a == per_dev - 1)
                def _():
                    @pl.when(has_right)
                    def _():
                        z_copy().wait_recv()
                        z_ref[per_dev - 1] = z_rcv[...]

                    @pl.when(jnp.logical_not(has_right))
                    def _():
                        z_ref[per_dev - 1, 0:4, :] = noise[step]

                    @pl.when(has_left)
                    def _():
                        z_copy().wait_send()

        def pre_s(j):
            @pl.when(ls == 0)
            def _():
                x_ref[j] = tdot(w_in[...], z_ref[j].astype(BF16)).astype(BF16).astype(F32)

        def post_s(j):
            @pl.when(has_right)
            def _():
                u_copy(0, par, j).start()

            @pl.when(has_left)
            def _():
                u_copy(1, par, j).start()

        def only_t(a, _):
            pre_t(a)
            run(a, (temporal_mlp(a, lt), T_COST))
            post_t(a)
            return 0

        def both(a, _):
            j = a - shift
            pre_t(a)
            pre_s(j)
            run(a, (temporal_mlp(a, lt), T_COST), (spatial(j, ls), S_COST))
            post_t(a)
            post_s(j)
            return 0

        def only_s(j, _):
            pre_s(j)
            run(j, (spatial(j, ls), S_COST))
            post_s(j)
            return 0

        end_t = lax.select(run_t, per_dev, 0)
        shift = lax.select(wrap, 2, 1)
        lone = lax.select(run_s, lax.min(shift, end_t), end_t)
        lax.fori_loop(0, lone, only_t, 0)
        lax.fori_loop(lone, end_t, both, 0)
        lax.fori_loop(lax.select(run_s, lax.max(end_t - shift, 0), per_dev), per_dev, only_s, 0)
        return 0

    lax.fori_loop(0, steps * layers + 1, body, 0)

    for f in range(per_dev):
        z_out[f] = z_ref[f, 0:4, :]

    @pl.when(has_left)
    def _():
        for s in range(steps):
            e_copy(s, 0).wait_recv()

    @pl.when(jnp.logical_not(has_left))
    def _():
        def fin(t, _):
            for s in range(steps):
                e_copy(s, t).wait_send()
            return 0
        lax.fori_loop(1, groups, fin, 0)

    mine = tok // groups
    for s in range(steps):
        e_out[s] = pltpu.roll(e_buf[s], tok - me * mine, 1)[:ch, :mine]


def solution(mesh):
    groups = mesh.shape['frames']
    slot_spec = P(('videos', 'frames'))

    def per_device(latents, slot_mod, step_dt, new_noise, w_in, spat_qkv, spat_out, temp_qkv, temp_out, temp_bias, w_up, w_down, w_out):
        per_dev, tok, ch = latents.shape
        layers, _, d, heads, hd = spat_qkv.shape
        steps = new_noise.shape[0]
        wide = w_up.shape[-1]
        window = temp_bias.shape[-1]
        radius = (window - 1) // 2

        z_t = jnp.swapaxes(latents, 1, 2)
        n_t = jnp.swapaxes(new_noise, 1, 2)
        mods = jnp.transpose(slot_mod, (1, 2, 0, 3))
        sq = jnp.transpose(spat_qkv, (0, 1, 3, 4, 2)).reshape(layers, 3 * d, d)
        tq = jnp.transpose(temp_qkv, (0, 1, 3, 4, 2)).reshape(layers, 3 * d, d)
        so = spat_out.reshape(layers, d, d)
        to = temp_out.reshape(layers, d, d)

        vm = pl.BlockSpec(memory_space=pltpu.VMEM)
        sm = pl.BlockSpec(memory_space=pltpu.SMEM)
        anys = pl.BlockSpec(memory_space=pl.ANY)
        V = pltpu.VMEM
        DMA = pltpu.SemaphoreType.DMA
        cfg = (groups, layers, steps, per_dev, heads, radius)
        e_all, z_fin = pl.pallas_call(
            functools.partial(kernel, cfg),
            out_shape=(jax.ShapeDtypeStruct((steps, ch, tok // groups), F32), jax.ShapeDtypeStruct((per_dev, ch, tok), F32)),
            in_specs=[vm, vm, vm, vm, vm, sm, sm] + [anys] * 6,
            out_specs=(vm, vm),
            scratch_shapes=[
                V((layers, 3 * d, d), BF16), V((layers, d, d), BF16), V((layers, 3 * d, d), BF16), V((layers, d, d), BF16),
                V((layers, d, wide), BF16), V((layers, wide, d), BF16), DMA((6, layers)),
                V((per_dev, d, tok), F32), V((per_dev, d, tok), BF16), V((2, 2, per_dev, d, tok), BF16),
                DMA((2, per_dev)), DMA((2, 2, per_dev)),
                V((per_dev, d, tok), BF16), V((2 * radius + per_dev, 2 * d, tok), BF16),
                V((3 * d, tok), BF16), V((d, tok), BF16), V((d, tok), BF16), V((d, tok), F32), V((d, tok), F32),
                V((heads, tok, tok), F32), V((heads, tok, tok), BF16), V((wide, tok), BF16),
                V((per_dev, window, tok // 128, 64, 128), F32), V((window, tok // 128, 8, 128), F32),
                V((per_dev, 8, tok), F32), V((8, tok), F32), V((8, tok), F32), DMA((2,)),
                V((steps, 8, tok), F32), DMA((steps, groups)), DMA((steps,)),
                V((layers, per_dev, d, 8), F32), V((layers, window, 8, 128), F32), V((8, d), BF16), V((8, d), BF16),
            ],
            compiler_params=pltpu.CompilerParams(has_side_effects=True, vmem_limit_bytes=64000000),
            name='fifo',
        )(z_t, n_t, mods, w_in, w_out.T, step_dt, temp_bias.reshape(-1), sq, so, tq, to, w_up, w_down)

        return jnp.swapaxes(e_all, 1, 2), jnp.swapaxes(z_fin, 1, 2)

    return jax.shard_map(per_device, mesh=mesh, in_specs=(slot_spec, slot_spec, slot_spec, P('videos'), P(), P(), P(), P(), P(), P(), P(), P(), P()), out_specs=(P('videos', 'frames'), slot_spec), check_vma=False)
```

```python
import functools
import math

import jax
import jax.numpy as jnp
from jax import lax
from jax.experimental import pallas as pl
from jax.experimental.pallas import tpu as pltpu
from jax.sharding import PartitionSpec as P

F32 = jnp.float32
BF16 = jnp.bfloat16
NORM_EPS = 1e-6
LOG2E = math.log2(math.e)
MESH = pl.DeviceIdType.MESH
NEG = -1e30


def tdot(lhs, rhs):
    return lax.dot_general(lhs, rhs, (((0,), (0,)), ((), ())), preferred_element_type=F32)


def dot(lhs, rhs):
    return jnp.dot(lhs, rhs, preferred_element_type=F32)


def fold(op, x, rows=8):
    n = x.shape[0] // 8
    k = 4 if n % 4 == 0 else 1
    parts = [x[i * 8:(i + 1) * 8] for i in range(n)]
    acc = parts[:k]
    for i in range(k, n):
        acc[i % k] = op(acc[i % k], parts[i])
    while len(acc) > 1:
        acc = [op(acc[i], acc[i + 1]) for i in range(0, len(acc) - 1, 2)] + ([acc[-1]] if len(acc) % 2 else [])
    return acc[0]


def gelu(x):
    half = 0.5 * x
    c = math.sqrt(2.0 / math.pi)
    return half + half * jnp.tanh(x * (c + (c * 0.044715) * (x * x)))


def kernel(cfg, z_in, noise, mods_in, w_in4, w_out4, dt, bias, sq_h, so_h, tq_h, to_h, up_h, dn_h,
           e_out, z_out,
           sq, so, tq, to, up, dn, wsem,
           x_ref, u_own, u_halo, send_sem, recv_sem,
           q_own, kv, qkv, o_s, o_t, x_s, x_t, s_ref, p_ref, hid, part, pp,
           z_ref, z_snd, z_rcv, zsem, e_buf, e_send, e_recv, mods, biasb, w_in, w_out):
    groups, layers, steps, per_dev, heads, radius = cfg
    d = x_ref.shape[1]
    tok = x_ref.shape[2]
    hd = d // heads
    wide = hid.shape[0]
    window = 2 * radius + 1
    lanes = 128
    chunks = tok // lanes
    scale = hd ** -0.5
    me = lax.axis_index('frames')
    left = lax.max(me - 1, 0)
    right = lax.min(me + 1, groups - 1)
    has_left = me > 0

    has_right = me < groups - 1

    pairs = ((sq_h, sq), (so_h, so), (tq_h, tq), (to_h, to), (up_h, up), (dn_h, dn))

    def wcopy(w, l):
        return pltpu.make_async_copy(pairs[w][0].at[l], pairs[w][1].at[l], wsem.at[w, l])

    barrier = pltpu.get_barrier_semaphore()

    @pl.when(has_left)
    def _():
        pl.semaphore_signal(barrier, inc=1, device_id={'frames': left}, device_id_type=MESH)

    @pl.when(has_right)
    def _():
        pl.semaphore_signal(barrier, inc=1, device_id={'frames': right}, device_id_type=MESH)

    @pl.when(me > 1)
    def _():
        pl.semaphore_signal(barrier, inc=1, device_id={'frames': 0}, device_id_type=MESH)

    for w in range(2):
        wcopy(w, 0).start()

    def u_copy(way, par, f):
        return pltpu.make_async_remote_copy(
            src_ref=u_own.at[f], dst_ref=u_halo.at[par, way, f],
            send_sem=send_sem.at[way, f], recv_sem=recv_sem.at[par, way, f],
            device_id={'frames': right if way == 0 else left}, device_id_type=MESH)

    def z_copy():
        return pltpu.make_async_remote_copy(
            src_ref=z_snd, dst_ref=z_rcv, send_sem=zsem.at[0], recv_sem=zsem.at[1],
            device_id={'frames': left}, device_id_type=MESH)

    def e_copy(s, t):
        return pltpu.make_async_remote_copy(
            src_ref=e_buf.at[s], dst_ref=e_buf.at[s], send_sem=e_send.at[s, t], recv_sem=e_recv.at[s],
            device_id={'frames': t}, device_id_type=MESH)

    ch = z_in.shape[1]
    w_in[...] = jnp.concatenate([w_in4[...].astype(F32), jnp.zeros((8 - ch, d), F32)], axis=0).astype(BF16)
    w_out[...] = jnp.concatenate([w_out4[...].astype(F32), jnp.zeros((8 - ch, d), F32)], axis=0).astype(BF16)

    @pl.when(has_left & has_right)
    def _():
        pl.semaphore_wait(barrier, 2)

    @pl.when(has_left & jnp.logical_not(has_right))
    def _():
        pl.semaphore_wait(barrier, 1)

    @pl.when(jnp.logical_not(has_left) & has_right)
    def _():
        pl.semaphore_wait(barrier, groups - 1)

    def prepare(l):
        for f in range(per_dev):
            rows = jnp.concatenate([mods_in[l, p, f:f + 1, :] for p in range(6)] + [jnp.zeros((2, d), F32)], axis=0)
            mods[l, f, :, 0:8] = jnp.transpose(rows)
        for j in range(window):
            biasb[l, j, 0:heads, :] = jnp.broadcast_to(bias[l, :, j:j + 1], (heads, lanes))

    biasb[...] = jnp.zeros_like(biasb)
    z_ref[...] = jnp.zeros_like(z_ref)
    for f in range(per_dev):
        z_ref[f, 0:4, :] = z_in[f]
    part[...] = jnp.zeros_like(part)

    @pl.when(jnp.logical_not(has_left))
    def _():
        u_halo[:, 0] = jnp.zeros((2,) + u_halo.shape[2:], BF16)

    @pl.when(jnp.logical_not(has_right))
    def _():
        u_halo[:, 1] = jnp.zeros((2,) + u_halo.shape[2:], BF16)

    def modulated(x, f, l, first):
        shift = mods[l, f, :, first:first + 1]
        gain = 1.0 + mods[l, f, :, first + 1:first + 2]
        out = []
        for c in range(chunks):
            part_x = x[:, c * lanes:(c + 1) * lanes]
            mean = jnp.sum(fold(jnp.add, part_x), axis=0, keepdims=True) * (1.0 / d)
            centred = part_x - mean
            var = jnp.sum(fold(jnp.add, centred * centred), axis=0, keepdims=True) * (1.0 / d)
            out.append((centred * lax.rsqrt(var + NORM_EPS) * gain + shift).astype(BF16))
        return jnp.concatenate(out, axis=1)

    def spatial(f, l):
        c_ln, c_qk, c_v, c_s, c_sm, c_pv, c_out, c_end = S_STEPS
        u = modulated(x_ref[f], f, l, 0)
        yield c_ln
        cut = 6

        def project(i):
            rows = slice(i * (3 * d // cut), (i + 1) * (3 * d // cut))
            qkv[rows, :] = dot(sq[l, rows, :], u).astype(BF16)

        early = cut if V_LATE == 0 else 2 * cut // 3
        for i in range(early):
            project(i)
            yield c_qk
        tops = []
        for h in range(heads):
            q = qkv[h * hd:(h + 1) * hd, :]
            k = qkv[d + h * hd:d + (h + 1) * hd, :]
            s = tdot(k, q)
            s_ref[h] = s
            tops.append(jnp.max(fold(jnp.maximum, s), axis=0, keepdims=True))
            yield c_s
        for i in range(early, cut):
            project(i)
            yield c_v
        for h in range(heads):
            for c in range(chunks):
                ln = slice(c * lanes, (c + 1) * lanes)
                s = s_ref[h, :, ln]
                e = jnp.exp2((s - tops[h][:, ln]) * (scale * LOG2E))
                total = jnp.sum(fold(jnp.add, e), axis=0, keepdims=True)
                p_ref[h, :, ln] = (e * (1.0 / total)).astype(BF16)
                yield c_sm // 2
        for h in range(heads):
            v = qkv[2 * d + h * hd:2 * d + (h + 1) * hd, :]
            o_s[h * hd:(h + 1) * hd, :] = dot(v, p_ref[h]).astype(BF16)
            yield c_pv
        x_s[...] = x_ref[f] + tdot(so[l], o_s[...])
        yield c_out
        u_own[f] = modulated(x_s[...], f, l, 2)
        x_ref[f] = x_s[...]
        yield c_end

    def scores(pairs):
        queries = sorted({a for _, qs in pairs for a in qs})
        for c in range(chunks):
            ln = slice(c * lanes, (c + 1) * lanes)
            for h in range(heads):
                hs = slice(h * hd, (h + 1) * hd)
                qf = {a: q_own[a, hs, ln].astype(F32) for a in queries}
                for key, qs in pairs:
                    kf = kv[key, hs, ln].astype(F32)
                    for a in qs:
                        part[a, key - a, c, h * 8:(h + 1) * 8, :] = fold(jnp.add, qf[a] * kf)
                yield 1

    def own(l):
        for f in range(0, per_dev, 2):
            u2 = jnp.concatenate([u_own[f], u_own[f + 1]], axis=1)
            for i in range(3):
                r = dot(tq[l, i * d:(i + 1) * d], u2).astype(BF16)
                for g in range(2):
                    if i == 0:
                        q_own[f + g] = r[:, g * tok:(g + 1) * tok]
                    else:
                        kv[radius + f + g, (i - 1) * d:i * d] = r[:, g * tok:(g + 1) * tok]
                yield 1

    def halo(l, par, blocks):
        for pair in blocks:
            u2 = jnp.concatenate([u_halo[par, way, f] for way, f in pair], axis=1)
            for i in range(2):
                r = dot(tq[l, (i + 1) * d:(i + 2) * d], u2).astype(BF16)
                for n, (way, f) in enumerate(pair):
                    kv[way * (radius + per_dev) + f, i * d:(i + 1) * d] = r[:, n * tok:(n + 1) * tok]
                yield 1

    def ahead(b, l, par):
        u = u_halo[par, 1, b]
        for i in range(4):
            rows = slice(i * (d // 2), (i + 1) * (d // 2))
            kv[radius + per_dev + b, rows] = dot(tq[l, d + i * (d // 2):d + (i + 1) * (d // 2)], u).astype(BF16)
            yield 100
        for c in range(chunks):
            ln = slice(c * lanes, (c + 1) * lanes)
            for h in range(heads):
                hs = slice(h * hd, (h + 1) * hd)
                qf = q_own[b, hs, ln].astype(F32)
                for key in (radius - 1, *range(radius + per_dev, radius + 2 * per_dev)):
                    kf = kv[key, hs, ln].astype(F32)
                    part[b, key - b, c, h * 8:(h + 1) * 8, :] = fold(jnp.add, qf * kf)
                yield 25

    def temporal_mlp(a, l):
        c_sm, c_pv, c_out, c_ln, c_up, c_gelu, c_down = T_STEPS
        first = me * per_dev + a - radius
        for c in range(chunks):
            ss = []
            for j in range(window):
                s = part[a, j, c, pl.ds(0, 8, stride=8), :]
                for r in range(1, 8):
                    s = s + part[a, j, c, pl.ds(r, 8, stride=8), :]
                ok = (first + j >= 0) & (first + j < groups * per_dev)
                ss.append(jnp.where(ok, s * scale + biasb[l, j], NEG))
            top = functools.reduce(jnp.maximum, ss)
            es = [jnp.exp(s - top) for s in ss]
            inv = 1.0 / functools.reduce(jnp.add, es)
            for j in range(window):
                pp[j, c] = (es[j] * inv).astype(BF16).astype(F32)
            yield c_sm
        for c in range(chunks):
            ln = slice(c * lanes, (c + 1) * lanes)
            for h in range(heads):
                acc = None
                for j in range(window):
                    vf = kv[a + j, d + h * hd:d + (h + 1) * hd, ln].astype(F32)
                    pb = pp[j, c, pl.ds(h, 8, stride=0), :]
                    t = jnp.concatenate([pb] * (hd // 8), axis=0) * vf
                    acc = t if acc is None else acc + t
                o_t[h * hd:(h + 1) * hd, ln] = acc.astype(BF16)
                yield c_pv
        x_t[...] = x_ref[a] + tdot(to[l], o_t[...])
        yield c_out
        u = modulated(x_t[...], a, l, 4)
        yield c_ln
        piece = d
        n = wide // piece
        hs = []
        for c in range(n + 1):
            if c < n:
                hs.append(tdot(up[l, :, c * piece:(c + 1) * piece], u))
                yield c_up
            if c > 0:
                hid[(c - 1) * piece:c * piece, :] = gelu(hs[c - 1]).astype(BF16)
                yield c_gelu
        x_ref[a] = x_t[...] + tdot(dn[l], hid[...])
        yield c_down

    def run(frame, *streams):
        live = [[g, total, 0.0] for g, total in streams]
        block = frame
        while live:
            block = block + 1

            @pl.when(lax.rem(block * (block + 1), 2) == 0)
            def _():
                waiting = list(live)
                while waiting:
                    entry = min(waiting, key=lambda t: t[2])
                    try:
                        cost = next(entry[0])
                    except StopIteration:
                        waiting.remove(entry)
                        live.remove(entry)
                        continue
                    if cost is None:
                        waiting.remove(entry)
                    else:
                        entry[2] += cost / entry[1]

    S_STEPS = (400, 50, 200, 160, 105, 112, 98, 800)
    T_STEPS = (117, 60, 196, 280, 400, 140, 1680)
    V_LATE = 0
    S_COST = 4784
    T_COST = 5270
    R_COST = 700

    def body(it, _):
        lt = lax.rem(it + layers - 1, layers)
        ls = lax.rem(it, layers)
        step = lax.div(it - 1, layers)
        par = lax.rem(it, 2)
        run_t = it > 0
        run_s = it < steps * layers
        wrap = (ls == 0) & run_t

        @pl.when(it < layers)
        def _():
            prepare(ls)
            for w in range(2):
                wcopy(w, ls).wait()

        @pl.when(it == 0)
        def _():
            for w in range(2, 6):
                wcopy(w, 0).start()

        @pl.when(it < layers - 1)
        def _():
            for w in range(6):
                wcopy(w, it + 1).start()

        @pl.when(run_t & (it <= layers))
        def _():
            for w in range(2, 6):
                wcopy(w, lt).wait()

        def arrived(f, ways=(0, 1)):
            for way in ways:
                @pl.when((has_left, has_right)[way])
                def _():
                    u_copy(way, 1 - par, f).wait_recv()

        @pl.when(run_t)
        def _():
            here = [(radius + f, range(per_dev)) for f in range(per_dev)]
            near = [(f, range(f + 1)) for f in range(per_dev)]
            run(it, (own(lt), 6))
            for f in range(per_dev - 1):
                arrived(f, (0,))
            arrived(0, (1,))
            run(it, (halo(lt, 1 - par, (((0, 0), (1, 0)), ((0, 1), (0, 2)))), 4), (scores(here), 12))
            arrived(per_dev - 1, (0,))
            run(it, (halo(lt, 1 - par, (((0, per_dev - 1),),)), 2), (scores(near[:-1] + [(radius + per_dev, (0,))]), 12))
            run(it + 1, (scores([(per_dev - 1, (0,))]), 12))

        def pre_t(a):
            @pl.when((a < per_dev - 1) & has_right)
            def _():
                u_copy(1, 1 - par, lax.min(a + 1, per_dev - 1)).wait_recv()

            @pl.when(has_right)
            def _():
                u_copy(0, 1 - par, a).wait_send()

            @pl.when(has_left)
            def _():
                u_copy(1, 1 - par, a).wait_send()

        def post_t(a):
            @pl.when(ls == 0)
            def _():
                v = dot(w_out[...], x_ref[a].astype(BF16))
                new = z_ref[a] + dt[a] * v

                @pl.when(a > 0)
                def _():
                    z_ref[a - 1] = new

                @pl.when((a == 0) & has_left)
                def _():
                    z_snd[...] = new

                @pl.when((a == 0) & jnp.logical_not(has_left))
                def _():
                    e_buf[step] = new

                @pl.when((a == 1) & has_left)
                def _():
                    z_copy().start()

                @pl.when((a == 1) & jnp.logical_not(has_left))
                def _():
                    def snd(t, _):
                        e_copy(step, t).start()
                        return 0
                    lax.fori_loop(1, groups, snd, 0)

                @pl.when(a == per_dev - 1)
                def _():
                    @pl.when(has_right)
                    def _():
                        z_copy().wait_recv()
                        z_ref[per_dev - 1] = z_rcv[...]

                    @pl.when(jnp.logical_not(has_right))
                    def _():
                        z_ref[per_dev - 1, 0:4, :] = noise[step]

                    @pl.when(has_left)
                    def _():
                        z_copy().wait_send()

        def pre_s(j):
            @pl.when(ls == 0)
            def _():
                x_ref[j] = tdot(w_in[...], z_ref[j].astype(BF16)).astype(BF16).astype(F32)

        def post_s(j):
            @pl.when(has_right)
            def _():
                u_copy(0, par, j).start()

            @pl.when(has_left)
            def _():
                u_copy(1, par, j).start()

        def only_t(a, _):
            pre_t(a)
            run(a, (temporal_mlp(a, lt), T_COST), (ahead(lax.min(a + 1, per_dev - 1), lt, 1 - par), R_COST))
            post_t(a)
            return 0

        def both(a, last):
            j = a - shift
            pre_t(a)
            pre_s(j)
            more = () if last else ((ahead(a + 1, lt, 1 - par), R_COST),)
            run(a, (temporal_mlp(a, lt), T_COST), (spatial(j, ls), S_COST), *more)
            post_t(a)
            post_s(j)

        def two(a, _):
            both(a, False)
            return 0

        def only_s(j, _):
            pre_s(j)
            run(j, (spatial(j, ls), S_COST))
            post_s(j)
            return 0

        end_t = lax.select(run_t, per_dev, 0)
        shift = lax.select(wrap, 2, 1)
        lone = lax.select(run_s, lax.min(shift, end_t), end_t)
        lax.fori_loop(0, lone, only_t, 0)
        lax.fori_loop(lone, lax.select(run_s, lax.max(end_t - 1, 0), lone), two, 0)

        @pl.when(run_t & run_s)
        def _():
            both(per_dev - 1, True)

        lax.fori_loop(lax.select(run_s, lax.max(end_t - shift, 0), per_dev), per_dev, only_s, 0)
        return 0

    lax.fori_loop(0, steps * layers + 1, body, 0)

    for f in range(per_dev):
        z_out[f] = z_ref[f, 0:4, :]

    @pl.when(has_left)
    def _():
        for s in range(steps):
            e_copy(s, 0).wait_recv()

    @pl.when(jnp.logical_not(has_left))
    def _():
        def fin(t, _):
            for s in range(steps):
                e_copy(s, t).wait_send()
            return 0
        lax.fori_loop(1, groups, fin, 0)

    mine = tok // groups
    for s in range(steps):
        e_out[s] = pltpu.roll(e_buf[s], tok - me * mine, 1)[:ch, :mine]


def solution(mesh):
    groups = mesh.shape['frames']
    slot_spec = P(('videos', 'frames'))

    def per_device(latents, slot_mod, step_dt, new_noise, w_in, spat_qkv, spat_out, temp_qkv, temp_out, temp_bias, w_up, w_down, w_out):
        per_dev, tok, ch = latents.shape
        layers, _, d, heads, hd = spat_qkv.shape
        steps = new_noise.shape[0]
        wide = w_up.shape[-1]
        window = temp_bias.shape[-1]
        radius = (window - 1) // 2

        z_t = jnp.swapaxes(latents, 1, 2)
        n_t = jnp.swapaxes(new_noise, 1, 2)
        mods = jnp.transpose(slot_mod, (1, 2, 0, 3))
        sq = jnp.transpose(spat_qkv, (0, 1, 3, 4, 2)).reshape(layers, 3 * d, d)
        tq = jnp.transpose(temp_qkv, (0, 1, 3, 4, 2)).reshape(layers, 3 * d, d)
        so = spat_out.reshape(layers, d, d)
        to = temp_out.reshape(layers, d, d)

        vm = pl.BlockSpec(memory_space=pltpu.VMEM)
        sm = pl.BlockSpec(memory_space=pltpu.SMEM)
        anys = pl.BlockSpec(memory_space=pl.ANY)
        V = pltpu.VMEM
        DMA = pltpu.SemaphoreType.DMA
        cfg = (groups, layers, steps, per_dev, heads, radius)
        e_all, z_fin = pl.pallas_call(
            functools.partial(kernel, cfg),
            out_shape=(jax.ShapeDtypeStruct((steps, ch, tok // groups), F32), jax.ShapeDtypeStruct((per_dev, ch, tok), F32)),
            in_specs=[vm, vm, vm, vm, vm, sm, vm] + [anys] * 6,
            out_specs=(vm, vm),
            scratch_shapes=[
                V((layers, 3 * d, d), BF16), V((layers, d, d), BF16), V((layers, 3 * d, d), BF16), V((layers, d, d), BF16),
                V((layers, d, wide), BF16), V((layers, wide, d), BF16), DMA((6, layers)),
                V((per_dev, d, tok), F32), V((per_dev, d, tok), BF16), V((2, 2, per_dev, d, tok), BF16),
                DMA((2, per_dev)), DMA((2, 2, per_dev)),
                V((per_dev, d, tok), BF16), V((2 * radius + per_dev, 2 * d, tok), BF16),
                V((3 * d, tok), BF16), V((d, tok), BF16), V((d, tok), BF16), V((d, tok), F32), V((d, tok), F32),
                V((heads, tok, tok), F32), V((heads, tok, tok), BF16), V((wide, tok), BF16),
                V((per_dev, window + per_dev - 1, tok // 128, 64, 128), F32), V((window, tok // 128, 8, 128), F32),
                V((per_dev, 8, tok), F32), V((8, tok), F32), V((8, tok), F32), DMA((2,)),
                V((steps, 8, tok), F32), DMA((steps, groups)), DMA((steps,)),
                V((layers, per_dev, d, 8), F32), V((layers, window, 8, 128), F32), V((8, d), BF16), V((8, d), BF16),
            ],
            compiler_params=pltpu.CompilerParams(has_side_effects=True, collective_id=0, vmem_limit_bytes=64000000),
            name='fifo',
        )(z_t, n_t, mods, w_in, w_out.T, step_dt, temp_bias, sq, so, tq, to, w_up, w_down)

        return jnp.swapaxes(e_all, 1, 2), jnp.swapaxes(z_fin, 1, 2)

    return jax.shard_map(per_device, mesh=mesh, in_specs=(slot_spec, slot_spec, slot_spec, P('videos'), P(), P(), P(), P(), P(), P(), P(), P(), P()), out_specs=(P('videos', 'frames'), slot_spec), check_vma=False)
```

```python
import functools
import math

import jax
import jax.numpy as jnp
from jax import lax
from jax.experimental import pallas as pl
from jax.experimental.pallas import tpu as pltpu
from jax.sharding import PartitionSpec as P

F32 = jnp.float32
BF16 = jnp.bfloat16
NORM_EPS = 1e-6
LOG2E = math.log2(math.e)
MESH = pl.DeviceIdType.MESH
NEG = -1e30


def tdot(lhs, rhs):
    return lax.dot_general(lhs, rhs, (((0,), (0,)), ((), ())), preferred_element_type=F32)


def dot(lhs, rhs):
    return jnp.dot(lhs, rhs, preferred_element_type=F32)


def fold(op, x, rows=8):
    n = x.shape[0] // 8
    k = 4 if n % 4 == 0 else 1
    parts = [x[i * 8:(i + 1) * 8] for i in range(n)]
    acc = parts[:k]
    for i in range(k, n):
        acc[i % k] = op(acc[i % k], parts[i])
    while len(acc) > 1:
        acc = [op(acc[i], acc[i + 1]) for i in range(0, len(acc) - 1, 2)] + ([acc[-1]] if len(acc) % 2 else [])
    return acc[0]


def gelu(x):
    half = 0.5 * x
    c = math.sqrt(2.0 / math.pi)
    return half + half * jnp.tanh(x * (c + (c * 0.044715) * (x * x)))


def kernel(cfg, z_in, noise, mods_in, w_in4, w_out4, dt, bias, sq_h, so_h, tq_h, to_h, up_h, dn_h,
           e_out, z_out,
           sq, so, tq, to, up, dn, wsem,
           x_ref, u_own, u_halo, send_sem, recv_sem,
           q_own, kv, qkv, o_s, o_t, x_s, x_t, s_ref, p_ref, hid, part, pp,
           z_ref, z_snd, z_rcv, zsem, e_buf, e_send, e_recv, mods, biasb, w_in, w_out):
    groups, layers, steps, per_dev, heads, radius = cfg
    d = x_ref.shape[1]
    tok = x_ref.shape[2]
    hd = d // heads
    wide = hid.shape[0]
    window = 2 * radius + 1
    lanes = 128
    chunks = tok // lanes
    scale = hd ** -0.5
    me = lax.axis_index('frames')
    left = lax.max(me - 1, 0)
    right = lax.min(me + 1, groups - 1)
    has_left = me > 0

    has_right = me < groups - 1

    pairs = ((sq_h, sq), (so_h, so), (tq_h, tq), (to_h, to), (up_h, up), (dn_h, dn))

    def wcopy(w, l):
        return pltpu.make_async_copy(pairs[w][0].at[l], pairs[w][1].at[l], wsem.at[w, l])

    barrier = pltpu.get_barrier_semaphore()

    @pl.when(has_left)
    def _():
        pl.semaphore_signal(barrier, inc=1, device_id={'frames': left}, device_id_type=MESH)

    @pl.when(has_right)
    def _():
        pl.semaphore_signal(barrier, inc=1, device_id={'frames': right}, device_id_type=MESH)

    @pl.when(me > 1)
    def _():
        pl.semaphore_signal(barrier, inc=1, device_id={'frames': 0}, device_id_type=MESH)

    for w in range(2):
        wcopy(w, 0).start()

    def u_copy(way, par, f):
        return pltpu.make_async_remote_copy(
            src_ref=u_own.at[f], dst_ref=u_halo.at[par, way, f],
            send_sem=send_sem.at[way, f], recv_sem=recv_sem.at[par, way, f],
            device_id={'frames': right if way == 0 else left}, device_id_type=MESH)

    def z_copy():
        return pltpu.make_async_remote_copy(
            src_ref=z_snd, dst_ref=z_rcv, send_sem=zsem.at[0], recv_sem=zsem.at[1],
            device_id={'frames': left}, device_id_type=MESH)

    def e_copy(s, t):
        return pltpu.make_async_remote_copy(
            src_ref=e_buf.at[s], dst_ref=e_buf.at[s], send_sem=e_send.at[s, t], recv_sem=e_recv.at[s],
            device_id={'frames': t}, device_id_type=MESH)

    ch = z_in.shape[1]
    w_in[...] = jnp.concatenate([w_in4[...].astype(F32), jnp.zeros((8 - ch, d), F32)], axis=0).astype(BF16)
    w_out[...] = jnp.concatenate([w_out4[...].astype(F32), jnp.zeros((8 - ch, d), F32)], axis=0).astype(BF16)

    @pl.when(has_left & has_right)
    def _():
        pl.semaphore_wait(barrier, 2)

    @pl.when(has_left & jnp.logical_not(has_right))
    def _():
        pl.semaphore_wait(barrier, 1)

    @pl.when(jnp.logical_not(has_left) & has_right)
    def _():
        pl.semaphore_wait(barrier, groups - 1)

    def prepare(l):
        for f in range(per_dev):
            rows = jnp.concatenate([mods_in[l, p, f:f + 1, :] + float(p % 2) for p in range(6)] + [jnp.zeros((2, d), F32)], axis=0)
            mods[l, f, :, 0:8] = jnp.transpose(rows)
        for j in range(window):
            biasb[l, j, 0:heads, :] = jnp.broadcast_to(bias[l, :, j:j + 1], (heads, lanes))

    biasb[...] = jnp.zeros_like(biasb)
    z_ref[...] = jnp.zeros_like(z_ref)
    for f in range(per_dev):
        z_ref[f, 0:4, :] = z_in[f]
    part[...] = jnp.zeros_like(part)

    @pl.when(jnp.logical_not(has_left))
    def _():
        u_halo[:, 0] = jnp.zeros((2,) + u_halo.shape[2:], BF16)

    @pl.when(jnp.logical_not(has_right))
    def _():
        u_halo[:, 1] = jnp.zeros((2,) + u_halo.shape[2:], BF16)

    def modulated(x, f, l, first):
        shift = mods[l, f, :, first:first + 1]
        gain = mods[l, f, :, first + 1:first + 2]
        out = []
        for c in range(chunks):
            part_x = x[:, c * lanes:(c + 1) * lanes]
            mean = jnp.sum(fold(jnp.add, part_x), axis=0, keepdims=True) * (1.0 / d)
            centred = part_x - mean
            var = jnp.sum(fold(jnp.add, centred * centred), axis=0, keepdims=True) * (1.0 / d)
            out.append((centred * lax.rsqrt(var + NORM_EPS) * gain + shift).astype(BF16))
        return jnp.concatenate(out, axis=1)

    def spatial(f, l, order):
        c_ln, c_qk, c_v, c_s, c_sm, c_pv, c_out, c_end = order
        u = modulated(x_ref[f], f, l, 0)
        yield c_ln
        cut = 6

        def project(i):
            rows = slice(i * (3 * d // cut), (i + 1) * (3 * d // cut))
            qkv[rows, :] = dot(sq[l, rows, :], u).astype(BF16)

        early = cut if V_LATE == 0 else 2 * cut // 3
        for i in range(early):
            project(i)
            yield c_qk
        tops = []
        for h in range(heads):
            q = qkv[h * hd:(h + 1) * hd, :]
            k = qkv[d + h * hd:d + (h + 1) * hd, :]
            s = tdot(k, q)
            s_ref[h] = s
            tops.append(jnp.max(fold(jnp.maximum, s), axis=0, keepdims=True))
            yield c_s
        for i in range(early, cut):
            project(i)
            yield c_v
        for h in range(heads):
            for c in range(chunks):
                ln = slice(c * lanes, (c + 1) * lanes)
                s = s_ref[h, :, ln]
                e = jnp.exp2((s - tops[h][:, ln]) * (scale * LOG2E))
                total = jnp.sum(fold(jnp.add, e), axis=0, keepdims=True)
                p_ref[h, :, ln] = (e * (1.0 / total)).astype(BF16)
                yield c_sm // 2
        for h in range(heads):
            v = qkv[2 * d + h * hd:2 * d + (h + 1) * hd, :]
            o_s[h * hd:(h + 1) * hd, :] = dot(v, p_ref[h]).astype(BF16)
            yield c_pv
        x_s[...] = x_ref[f] + tdot(so[l], o_s[...])
        yield c_out
        u_own[f] = modulated(x_s[...], f, l, 2)
        x_ref[f] = x_s[...]
        yield c_end

    def scores(pairs):
        queries = sorted({a for _, qs in pairs for a in qs})
        for c in range(chunks):
            ln = slice(c * lanes, (c + 1) * lanes)
            for h in range(heads):
                hs = slice(h * hd, (h + 1) * hd)
                qf = {a: q_own[a, hs, ln].astype(F32) for a in queries}
                for key, qs in pairs:
                    kf = kv[key, hs, ln].astype(F32)
                    for a in qs:
                        part[a, key - a, c, h * 8:(h + 1) * 8, :] = fold(jnp.add, qf[a] * kf)
                yield 1

    def own(l):
        for f in range(0, per_dev, 2):
            u2 = jnp.concatenate([u_own[f], u_own[f + 1]], axis=1)
            for i in range(3):
                r = dot(tq[l, i * d:(i + 1) * d], u2).astype(BF16)
                for g in range(2):
                    if i == 0:
                        q_own[f + g] = r[:, g * tok:(g + 1) * tok]
                    else:
                        kv[radius + f + g, (i - 1) * d:i * d] = r[:, g * tok:(g + 1) * tok]
                yield 1

    def halo(l, par, blocks):
        for pair in blocks:
            u2 = jnp.concatenate([u_halo[par, way, f] for way, f in pair], axis=1)
            for i in range(2):
                r = dot(tq[l, (i + 1) * d:(i + 2) * d], u2).astype(BF16)
                for n, (way, f) in enumerate(pair):
                    kv[way * (radius + per_dev) + f, i * d:(i + 1) * d] = r[:, n * tok:(n + 1) * tok]
                yield 1

    def ahead(b, l, par):
        u = u_halo[par, 1, b]
        for i in range(4):
            rows = slice(i * (d // 2), (i + 1) * (d // 2))
            kv[radius + per_dev + b, rows] = dot(tq[l, d + i * (d // 2):d + (i + 1) * (d // 2)], u).astype(BF16)
            yield 100
        for c in range(chunks):
            ln = slice(c * lanes, (c + 1) * lanes)
            for h in range(heads):
                hs = slice(h * hd, (h + 1) * hd)
                qf = q_own[b, hs, ln].astype(F32)
                for key in (radius - 1, *range(radius + per_dev, radius + 2 * per_dev)):
                    kf = kv[key, hs, ln].astype(F32)
                    part[b, key - b, c, h * 8:(h + 1) * 8, :] = fold(jnp.add, qf * kf)
                yield 25

    def temporal_mlp(a, l, order):
        piece, c_sm, c_pv, c_out, c_ln, c_up, c_gelu, c_down = order
        first = me * per_dev + a - radius
        for c in range(chunks):
            ss = []
            for j in range(window):
                s = part[a, j, c, pl.ds(0, 8, stride=8), :]
                for r in range(1, 8):
                    s = s + part[a, j, c, pl.ds(r, 8, stride=8), :]
                ok = (first + j >= 0) & (first + j < groups * per_dev)
                ss.append(jnp.where(ok, s * scale + biasb[l, j], NEG))
            top = functools.reduce(jnp.maximum, ss)
            es = [jnp.exp(s - top) for s in ss]
            inv = 1.0 / functools.reduce(jnp.add, es)
            for j in range(window):
                pp[j, c] = (es[j] * inv).astype(BF16).astype(F32)
            yield c_sm
        for c in range(chunks):
            ln = slice(c * lanes, (c + 1) * lanes)
            for h in range(heads):
                acc = None
                for j in range(window):
                    vf = kv[a + j, d + h * hd:d + (h + 1) * hd, ln].astype(F32)
                    pb = pp[j, c, pl.ds(h, 8, stride=0), :]
                    t = jnp.concatenate([pb] * (hd // 8), axis=0) * vf
                    acc = t if acc is None else acc + t
                o_t[h * hd:(h + 1) * hd, ln] = acc.astype(BF16)
                yield c_pv
        x_t[...] = x_ref[a] + tdot(to[l], o_t[...])
        yield c_out
        u = modulated(x_t[...], a, l, 4)
        yield c_ln
        n = wide // piece
        hs = []
        for c in range(n + 1):
            if c < n:
                hs.append(tdot(up[l, :, c * piece:(c + 1) * piece], u))
                yield c_up
            if c > 0:
                hid[(c - 1) * piece:c * piece, :] = gelu(hs[c - 1]).astype(BF16)
                yield c_gelu
        x_ref[a] = x_t[...] + tdot(dn[l], hid[...])
        yield c_down

    def run(frame, *streams):
        live = [[g, total, 0.0] for g, total in streams]
        block = frame
        while live:
            block = block + 1

            @pl.when(lax.rem(block * (block + 1), 2) == 0)
            def _():
                waiting = list(live)
                while waiting:
                    entry = min(waiting, key=lambda t: t[2])
                    try:
                        cost = next(entry[0])
                    except StopIteration:
                        waiting.remove(entry)
                        live.remove(entry)
                        continue
                    if cost is None:
                        waiting.remove(entry)
                    else:
                        entry[2] += cost / entry[1]

    V_LATE = 0
    S_STEPS, S_COST = (400, 50, 200, 160, 105, 112, 98, 800), 4784
    T_STEPS, T_COST = (d, 117, 60, 196, 280, 400, 140, 1680), 5270
    S_TWO, S_TWO_COST = (800, 100, 100, 224, 105, 112, 137, 1600), 8674
    T_TWO, T_TWO_COST = (d, 81, 60, 98, 280, 200, 70, 840), 3180
    R_COST = 900
    T_LONE, T_LONE_COST = (d // 2, 165, 96, 19, 200, 422, 220, 750), 7587
    R_LONE_COST = 400

    def body(it, _):
        lt = lax.rem(it + layers - 1, layers)
        ls = lax.rem(it, layers)
        step = lax.div(it - 1, layers)
        par = lax.rem(it, 2)
        run_t = it > 0
        run_s = it < steps * layers
        wrap = (ls == 0) & run_t

        @pl.when(it < layers)
        def _():
            prepare(ls)
            for w in range(2):
                wcopy(w, ls).wait()

        @pl.when(it == 0)
        def _():
            for w in range(2, 6):
                wcopy(w, 0).start()

        @pl.when(it < layers - 1)
        def _():
            for w in range(6):
                wcopy(w, it + 1).start()

        @pl.when(run_t & (it <= layers))
        def _():
            for w in range(2, 6):
                wcopy(w, lt).wait()

        def arrived(f, ways=(0, 1)):
            for way in ways:
                @pl.when((has_left, has_right)[way])
                def _():
                    u_copy(way, 1 - par, f).wait_recv()

        @pl.when(run_t)
        def _():
            here = [(radius + f, range(per_dev)) for f in range(per_dev)]
            near = [(f, range(f + 1)) for f in range(per_dev)]
            run(it, (own(lt), 6))
            for f in range(per_dev - 1):
                arrived(f, (0,))
            arrived(0, (1,))
            run(it, (halo(lt, 1 - par, (((0, 0), (1, 0)), ((0, 1), (0, 2)))), 4), (scores(here), 12))
            arrived(per_dev - 1, (0,))
            run(it, (halo(lt, 1 - par, (((0, per_dev - 1),),)), 2), (scores(near[:-1] + [(radius + per_dev, (0,))]), 12))
            run(it + 1, (scores([(per_dev - 1, (0,))]), 12))

        def pre_t(a):
            @pl.when((a < per_dev - 1) & has_right)
            def _():
                u_copy(1, 1 - par, lax.min(a + 1, per_dev - 1)).wait_recv()

            @pl.when(has_right)
            def _():
                u_copy(0, 1 - par, a).wait_send()

            @pl.when(has_left)
            def _():
                u_copy(1, 1 - par, a).wait_send()

        def post_t(a):
            @pl.when(ls == 0)
            def _():
                v = dot(w_out[...], x_ref[a].astype(BF16))
                new = z_ref[a] + dt[a] * v

                @pl.when(a > 0)
                def _():
                    z_ref[a - 1] = new

                @pl.when((a == 0) & has_left)
                def _():
                    z_snd[...] = new

                @pl.when((a == 0) & jnp.logical_not(has_left))
                def _():
                    e_buf[step] = new

                @pl.when((a == 1) & has_left)
                def _():
                    z_copy().start()

                @pl.when((a == 1) & jnp.logical_not(has_left))
                def _():
                    def snd(t, _):
                        e_copy(step, t).start()
                        return 0
                    lax.fori_loop(1, groups, snd, 0)

                @pl.when(a == per_dev - 1)
                def _():
                    @pl.when(has_right)
                    def _():
                        z_copy().wait_recv()
                        z_ref[per_dev - 1] = z_rcv[...]

                    @pl.when(jnp.logical_not(has_right))
                    def _():
                        z_ref[per_dev - 1, 0:4, :] = noise[step]

                    @pl.when(has_left)
                    def _():
                        z_copy().wait_send()

        def pre_s(j):
            @pl.when(ls == 0)
            def _():
                x_ref[j] = tdot(w_in[...], z_ref[j].astype(BF16)).astype(BF16).astype(F32)

        def post_s(j):
            @pl.when(has_right)
            def _():
                u_copy(0, par, j).start()

            @pl.when(has_left)
            def _():
                u_copy(1, par, j).start()

        def only_t(a, _):
            pre_t(a)
            run(a, (temporal_mlp(a, lt, T_LONE), T_LONE_COST), (ahead(lax.min(a + 1, per_dev - 1), lt, 1 - par), R_LONE_COST))
            post_t(a)
            return 0

        def both(a, last):
            j = a - shift
            pre_t(a)
            pre_s(j)
            if last:
                run(a, (temporal_mlp(a, lt, T_STEPS), T_COST), (spatial(j, ls, S_STEPS), S_COST))
            else:
                run(a, (temporal_mlp(a, lt, T_TWO), T_TWO_COST), (spatial(j, ls, S_TWO), S_TWO_COST), (ahead(a + 1, lt, 1 - par), R_COST))
            post_t(a)
            post_s(j)

        def two(a, _):
            both(a, False)
            return 0

        def only_s(j, _):
            pre_s(j)
            run(j, (spatial(j, ls, S_STEPS), S_COST))
            post_s(j)
            return 0

        end_t = lax.select(run_t, per_dev, 0)
        shift = lax.select(wrap, 2, 1)
        lone = lax.select(run_s, lax.min(shift, end_t), end_t)
        lax.fori_loop(0, lone, only_t, 0)
        lax.fori_loop(lone, lax.select(run_s, lax.max(end_t - 1, 0), lone), two, 0)

        @pl.when(run_t & run_s)
        def _():
            both(per_dev - 1, True)

        lax.fori_loop(lax.select(run_s, lax.max(end_t - shift, 0), per_dev), per_dev, only_s, 0)
        return 0

    lax.fori_loop(0, steps * layers + 1, body, 0)

    for f in range(per_dev):
        z_out[f] = z_ref[f, 0:4, :]

    @pl.when(has_left)
    def _():
        for s in range(steps):
            e_copy(s, 0).wait_recv()

    @pl.when(jnp.logical_not(has_left))
    def _():
        def fin(t, _):
            for s in range(steps):
                e_copy(s, t).wait_send()
            return 0
        lax.fori_loop(1, groups, fin, 0)

    mine = tok // groups
    for s in range(steps):
        e_out[s] = pltpu.roll(e_buf[s], tok - me * mine, 1)[:ch, :mine]


def solution(mesh):
    groups = mesh.shape['frames']
    slot_spec = P(('videos', 'frames'))

    def per_device(latents, slot_mod, step_dt, new_noise, w_in, spat_qkv, spat_out, temp_qkv, temp_out, temp_bias, w_up, w_down, w_out):
        per_dev, tok, ch = latents.shape
        layers, _, d, heads, hd = spat_qkv.shape
        steps = new_noise.shape[0]
        wide = w_up.shape[-1]
        window = temp_bias.shape[-1]
        radius = (window - 1) // 2

        z_t = jnp.swapaxes(latents, 1, 2)
        n_t = jnp.swapaxes(new_noise, 1, 2)
        mods = jnp.transpose(slot_mod, (1, 2, 0, 3))
        sq = jnp.transpose(spat_qkv, (0, 1, 3, 4, 2)).reshape(layers, 3 * d, d)
        tq = jnp.transpose(temp_qkv, (0, 1, 3, 4, 2)).reshape(layers, 3 * d, d)
        so = spat_out.reshape(layers, d, d)
        to = temp_out.reshape(layers, d, d)

        vm = pl.BlockSpec(memory_space=pltpu.VMEM)
        sm = pl.BlockSpec(memory_space=pltpu.SMEM)
        anys = pl.BlockSpec(memory_space=pl.ANY)
        V = pltpu.VMEM
        DMA = pltpu.SemaphoreType.DMA
        cfg = (groups, layers, steps, per_dev, heads, radius)
        e_all, z_fin = pl.pallas_call(
            functools.partial(kernel, cfg),
            out_shape=(jax.ShapeDtypeStruct((steps, ch, tok // groups), F32), jax.ShapeDtypeStruct((per_dev, ch, tok), F32)),
            in_specs=[vm, vm, vm, vm, vm, sm, vm] + [anys] * 6,
            out_specs=(vm, vm),
            scratch_shapes=[
                V((layers, 3 * d, d), BF16), V((layers, d, d), BF16), V((layers, 3 * d, d), BF16), V((layers, d, d), BF16),
                V((layers, d, wide), BF16), V((layers, wide, d), BF16), DMA((6, layers)),
                V((per_dev, d, tok), F32), V((per_dev, d, tok), BF16), V((2, 2, per_dev, d, tok), BF16),
                DMA((2, per_dev)), DMA((2, 2, per_dev)),
                V((per_dev, d, tok), BF16), V((2 * radius + per_dev, 2 * d, tok), BF16),
                V((3 * d, tok), BF16), V((d, tok), BF16), V((d, tok), BF16), V((d, tok), F32), V((d, tok), F32),
                V((heads, tok, tok), F32), V((heads, tok, tok), BF16), V((wide, tok), BF16),
                V((per_dev, window + per_dev - 1, tok // 128, 64, 128), F32), V((window, tok // 128, 8, 128), F32),
                V((per_dev, 8, tok), F32), V((8, tok), F32), V((8, tok), F32), DMA((2,)),
                V((steps, 8, tok), F32), DMA((steps, groups)), DMA((steps,)),
                V((layers, per_dev, d, 8), F32), V((layers, window, 8, 128), F32), V((8, d), BF16), V((8, d), BF16),
            ],
            compiler_params=pltpu.CompilerParams(has_side_effects=True, collective_id=0, vmem_limit_bytes=64000000),
            name='fifo',
        )(z_t, n_t, mods, w_in, w_out.T, step_dt, temp_bias, sq, so, tq, to, w_up, w_down)

        return jnp.swapaxes(e_all, 1, 2), jnp.swapaxes(z_fin, 1, 2)

    return jax.shard_map(per_device, mesh=mesh, in_specs=(slot_spec, slot_spec, slot_spec, P('videos'), P(), P(), P(), P(), P(), P(), P(), P(), P()), out_specs=(P('videos', 'frames'), slot_spec), check_vma=False)
```
